32 devices in a mesh: row: 8 (over z, y), ta: 4 (over x, core).
Axes of the slice: x: 2, y: 2, z: 4, core: 2. Of those that a mesh axis runs over, the one named last changes fastest.
Arguments:
- hidden: bfloat16 [8, 256, 3584], P('row', None, 'ta'), may hold values from -6 to 6
- target: bfloat16 [8, 256, 3584], P('row', None, 'ta'), may hold values from -6 to 6
- w_down: bfloat16 [8, 2, 3584, 256], P('row', None, 'ta'), may hold values from -5 to 5
- w_up: bfloat16 [8, 2, 256, 3584], P('row', None, None, 'ta'), may hold values from -5 to 5
- m_down: float32 [8, 2, 3584, 256], P('row', None, 'ta'), may hold values from -9 to 9
- m_up: float32 [8, 2, 256, 3584], P('row', None, None, 'ta'), may hold values from -9 to 9
Outputs:
- avg_down: bfloat16 [2, 3584, 256], P(None, 'ta')
- avg_up: bfloat16 [2, 256, 3584], P(None, None, 'ta')
- mom_down: float32 [2, 3584, 256], P(None, 'ta')
- mom_up: float32 [2, 256, 3584], P(None, None, 'ta')
The draws below stay inside these ranges and needn't reach their ends.
All inputs are finite; a program needn't handle non-finite values.
Results may differ from the reference program's by a relative error of at most 0.019.
Values may be sent and summed in bfloat16 or wider, within the bound.
No kernel may reach another device: no remote copies, remote signals or barrier semaphores. Data moves between devices by JAX's collectives and lax.ppermute only.
A program may use at most 128 MiB of HBM per device.

```python
import jax
import jax.numpy as jnp
from jax import lax

D = 3584
RANK = 256
LAYERS = 2
STEPS = 4
TOK = 256
REPLICAS = 8


def draw_hidden(key, part):
    values = jax.random.truncated_normal(jax.random.fold_in(key, 11), -6.0, 6.0, (REPLICAS, TOK, D), jnp.float32)
    return values.astype(jnp.bfloat16)


def draw_target(key, part):
    values = jax.random.truncated_normal(jax.random.fold_in(key, 12), -6.0, 6.0, (REPLICAS, TOK, D), jnp.float32)
    return values.astype(jnp.bfloat16)


def draw_w_down(key, part):
    values = jax.random.truncated_normal(jax.random.fold_in(key, 13), -5.0, 5.0, (REPLICAS, LAYERS, D, RANK), jnp.float32)
    return values.astype(jnp.bfloat16)


def draw_w_up(key, part):
    values = jax.random.truncated_normal(jax.random.fold_in(key, 14), -5.0, 5.0, (REPLICAS, LAYERS, RANK, D), jnp.float32)
    return values.astype(jnp.bfloat16)


def draw_m_down(key, part):
    values = 1.5 * jax.random.truncated_normal(jax.random.fold_in(key, 15), -6.0, 6.0, (REPLICAS, LAYERS, D, RANK), jnp.float32)
    return values.astype(jnp.float32)


def draw_m_up(key, part):
    values = 1.5 * jax.random.truncated_normal(jax.random.fold_in(key, 16), -6.0, 6.0, (REPLICAS, LAYERS, RANK, D), jnp.float32)
    return values.astype(jnp.float32)


def setup_inputs(seed: int = 0) -> dict:
    seeds = jax.random.split(jax.random.key(seed), 7)
    return {
        "hidden": draw_hidden(jax.random.fold_in(seeds[6], 71), 0),
        "target": draw_target(jax.random.fold_in(seeds[6], 71), 0),
        "w_down": draw_w_down(jax.random.fold_in(seeds[6], 71), 0),
        "w_up": draw_w_up(jax.random.fold_in(seeds[6], 71), 0),
        "m_down": draw_m_down(jax.random.fold_in(seeds[6], 71), 0),
        "m_up": draw_m_up(jax.random.fold_in(seeds[6], 71), 0),
    }


norm_eps = 1e-06
learn_rate = 0.02
moment_decay = 0.9

def silu_slope(preact):
    sigmoid_v = jax.nn.sigmoid(preact)
    return sigmoid_v * (1.0 + preact * (1.0 - sigmoid_v))

def replica_steps(hidden, target, w_down, w_up, m_down, m_up):
    for step_index in range(STEPS):
        stored = []
        current = hidden
        for layer_index in range(LAYERS):
            wide_rows = current.astype(jnp.float32)
            root_mean = jnp.sqrt(lax.optimization_barrier(jnp.mean(wide_rows * wide_rows, axis=1, keepdims=True)) + norm_eps)
            projected = jnp.dot(current, w_down[layer_index], preferred_element_type=jnp.float32) * D ** (-0.5)
            preact = projected / root_mean
            activation = jax.nn.silu(preact).astype(jnp.bfloat16)
            stored.append((current, root_mean, preact, activation))
            lifted = jnp.dot(activation, w_up[layer_index], preferred_element_type=jnp.float32) * RANK ** (-0.5)
            current = (wide_rows + lifted).astype(jnp.bfloat16)
        gradient = current.astype(jnp.float32) - target.astype(jnp.float32)
        grads_down = [None] * LAYERS
        grads_up = [None] * LAYERS
        for layer_index in reversed(range(LAYERS)):
            current, root_mean, preact, activation = stored[layer_index]
            grad_low = gradient.astype(jnp.bfloat16)
            grads_up[layer_index] = jnp.dot(activation.T, grad_low, preferred_element_type=jnp.float32) * RANK ** (-0.5)
            grad_act = jnp.dot(grad_low, w_up[layer_index].T, preferred_element_type=jnp.float32) * RANK ** (-0.5)
            grad_pre = grad_act * silu_slope(preact)
            row_dot = lax.optimization_barrier(jnp.sum(grad_pre * preact, axis=1, keepdims=True))
            grad_proj = (grad_pre / root_mean).astype(jnp.bfloat16)
            grads_down[layer_index] = jnp.dot(current.T, grad_proj, preferred_element_type=jnp.float32) * D ** (-0.5)
            wide_rows = current.astype(jnp.float32)
            through = jnp.dot(grad_proj, w_down[layer_index].T, preferred_element_type=jnp.float32) * D ** (-0.5)
            gradient = gradient + through - row_dot * wide_rows / (D * root_mean * root_mean)
        m_down = moment_decay * m_down + jnp.stack(grads_down)
        m_up = moment_decay * m_up + jnp.stack(grads_up)
        w_down = (w_down.astype(jnp.float32) - learn_rate * m_down).astype(jnp.bfloat16)
        w_up = (w_up.astype(jnp.float32) - learn_rate * m_up).astype(jnp.bfloat16)
    return (w_down, w_up, m_down, m_up)

def accumulate(totals, inputs):
    finals = replica_steps(inputs[0], inputs[1], inputs[2], inputs[3], inputs[4], inputs[5])
    return (tuple((total + final.astype(jnp.float32) for total, final in zip(totals, finals))), None)

def reference(hidden, target, w_down, w_up, m_down, m_up):
    replicas = hidden.shape[0]
    zeros_init = (jnp.zeros(w_down.shape[1:], jnp.float32), jnp.zeros(w_up.shape[1:], jnp.float32), jnp.zeros(m_down.shape[1:], jnp.float32), jnp.zeros(m_up.shape[1:], jnp.float32))
    totals, unused = lax.scan(accumulate, zeros_init, (hidden, target, w_down, w_up, m_down, m_up))
    avg_down = (totals[0] / replicas).astype(jnp.bfloat16)
    avg_up = (totals[1] / replicas).astype(jnp.bfloat16)
    return (avg_down, avg_up, totals[2] / replicas, totals[3] / replicas)
```

```python
import jax
import jax.numpy as jnp
from jax import lax
from jax.sharding import PartitionSpec as P

STEPS = 4

norm_eps = 1e-06
learn_rate = 0.02
moment_decay = 0.9

f32 = jnp.float32
bf16 = jnp.bfloat16


def dot(a, b, dim_a=1, dim_b=0):
    return lax.dot_general(a, b, (((dim_a,), (dim_b,)), ((), ())), preferred_element_type=f32)


def exchange_sum(parts, axis):
    size = lax.axis_size(axis)
    if size & (size - 1):
        return [lax.psum(p, axis).astype(f32) for p in parts]
    stride = 1
    while stride < size:
        pairs = [(i, i ^ stride) for i in range(size)]
        others = [lax.ppermute(p, axis, pairs) for p in parts]
        sums = [p.astype(f32) + o.astype(f32) for p, o in zip(parts, others)]
        stride *= 2
        if stride < size:
            parts = [s.astype(p.dtype) for s, p in zip(sums, parts)]
    return sums


def ring_order(size):
    return list(range(0, size, 2)) + list(range(size - 1 - size % 2, 0, -2))


def ring_average(arrays, outs, axis):
    size = lax.axis_size(axis)
    order = ring_order(size)
    place = [0] * size
    for k, d in enumerate(order):
        place[d] = k
    me = jnp.asarray(place, jnp.int32)[lax.axis_index(axis)]
    ahead = [(order[k], order[(k + 1) % size]) for k in range(size)]
    back = [(b, a) for a, b in ahead]
    flows = []
    for j, a in enumerate(arrays):
        rows = a.shape[0] // size
        flows.append((ahead, 1, a, rows) if j % 2 == 0 else (back, -1, a, rows))

    def shard(a, k, rows):
        return lax.dynamic_slice_in_dim(a, (k % size) * rows, rows, 0)

    held = [shard(a, me - sign, rows).astype(bf16) for _, sign, a, rows in flows]
    for hop in range(1, size):
        moved = [lax.ppermute(h, axis, f[0]) for h, f in zip(held, flows)]
        held = []
        for m, (_, sign, a, rows) in zip(moved, flows):
            own = shard(a, me - sign * (hop + 1), rows)
            total = m.astype(f32) + own.astype(f32)
            if hop == size - 1:
                total = total / size
            held.append(total.astype(bf16))
    results = []
    for h, (_, sign, a, rows), o in zip(held, flows, outs):
        results.append(lax.dynamic_update_slice_in_dim(jnp.zeros(a.shape, o), h.astype(o), me * rows, 0))
    for hop in range(1, size):
        held = [lax.ppermute(h, axis, f[0]) for h, f in zip(held, flows)]
        for j, (h, (_, sign, a, rows), o) in enumerate(zip(held, flows, outs)):
            at = ((me - sign * hop) % size) * rows
            results[j] = lax.dynamic_update_slice_in_dim(results[j], h.astype(o), at, 0)
    return results


def column_sums(x):
    wide = x.astype(f32)
    return jnp.sum(wide * wide, axis=1)


def slope(pre, sig):
    return sig * (1.0 + pre * (1.0 - sig))


def body(hidden, target, w_down, w_up, m_down, m_up):
    x0, goal = hidden[0], target[0]
    wd = [w_down[0, 0], w_down[0, 1]]
    wu = [w_up[0, 0], w_up[0, 1]]
    md = [m_down[0, 0], m_down[0, 1]]
    mu = [m_up[0, 0], m_up[0, 1]]
    width = x0.shape[1] * lax.axis_size("ta")
    rank = wu[0].shape[0]
    cd, cu = width**-0.5, rank**-0.5

    proj0, drift0, gram0, square0 = exchange_sum(
        [
            dot(x0, wd[0]).astype(bf16),
            dot(x0, md[0].astype(bf16)).astype(bf16),
            dot(x0, x0, 1, 1).astype(bf16),
            column_sums(x0),
        ],
        "ta",
    )
    rms0 = jnp.sqrt(square0 / width + norm_eps)[:, None]
    gram0 = gram0.astype(bf16)

    for step in range(STEPS):
        pre0 = proj0 * cd / rms0
        sig0 = jax.nn.sigmoid(pre0)
        act0 = (pre0 * sig0).astype(bf16)
        x1 = (x0.astype(f32) + dot(act0, wu[0]) * cu).astype(bf16)
        proj1, square1 = exchange_sum([dot(x1, wd[1]).astype(bf16), column_sums(x1)], "ta")
        cross, low = exchange_sum(
            [dot(wu[0], wd[1]).astype(bf16), dot(x1, wu[0], 1, 1).astype(bf16)], "ta"
        )
        rms1 = jnp.sqrt(square1 / width + norm_eps)[:, None]
        pre1 = proj1 * cd / rms1
        sig1 = jax.nn.sigmoid(pre1)
        act1 = (pre1 * sig1).astype(bf16)
        x2 = (x1.astype(f32) + dot(act1, wu[1]) * cu).astype(bf16)
        grad2 = x2.astype(f32) - goal.astype(f32)
        gb1 = grad2.astype(bf16)
        back1, back0 = exchange_sum(
            [dot(gb1, wu[1], 1, 1).astype(bf16), dot(gb1, wu[0], 1, 1).astype(bf16)], "ta"
        )
        g_pre1 = back1 * cu * slope(pre1, sig1)
        row_dot1 = jnp.sum(g_pre1 * pre1, axis=1, keepdims=True)
        g_proj1 = (g_pre1 / rms1).astype(bf16)
        pull1 = row_dot1 / (width * rms1 * rms1)
        grad1 = grad2 + dot(g_proj1, wd[1], 1, 1) * cd - pull1 * x1.astype(f32)
        gb0 = grad1.astype(bf16)
        g_act0 = (back0 + dot(g_proj1, cross.astype(bf16), 1, 1) * cd - pull1 * low) * cu
        g_proj0 = (g_act0 * slope(pre0, sig0) / rms0).astype(bf16)
        g_up = [dot(act0, gb0, 0, 0) * cu, dot(act1, gb1, 0, 0) * cu]
        g_down = [dot(x0, g_proj0, 0, 0) * cd, dot(x1, g_proj1, 0, 0) * cd]
        mu = [moment_decay * m + g for m, g in zip(mu, g_up)]
        md = [moment_decay * m + g for m, g in zip(md, g_down)]
        wu = [(w.astype(f32) - learn_rate * m).astype(bf16) for w, m in zip(wu, mu)]
        wd = [(w.astype(f32) - learn_rate * m).astype(bf16) for w, m in zip(wd, md)]
        drift0 = moment_decay * drift0 + dot(gram0, g_proj0) * cd
        proj0 = proj0 - learn_rate * drift0

    def flat(pair):
        return jnp.concatenate(pair, axis=0)

    wd, wu, md, mu = ring_average(
        [flat(wd), flat(wu), flat(md), flat(mu)], [bf16, bf16, f32, f32], "row"
    )
    down, up = w_down.shape[1:], w_up.shape[1:]
    return (wd.reshape(down), wu.reshape(up), md.reshape(down), mu.reshape(up))


def solution(mesh):
    placed = (
        P("row", None, "ta"),
        P("row", None, "ta"),
        P("row", None, "ta", None),
        P("row", None, None, "ta"),
        P("row", None, "ta", None),
        P("row", None, None, "ta"),
    )
    return jax.shard_map(
        body,
        mesh=mesh,
        in_specs=placed,
        out_specs=(
            P(None, "ta", None),
            P(None, None, "ta"),
            P(None, "ta", None),
            P(None, None, "ta"),
        ),
        check_vma=False,
    )
```

```python
import jax
import jax.numpy as jnp
from jax import lax
from jax.experimental import pallas as pl
from jax.experimental.pallas import tpu as pltpu
from jax.sharding import PartitionSpec as P

STEPS = 4
LONG_RING = 16

norm_eps = 1e-06
learn_rate = 0.02
moment_decay = 0.9

f32 = jnp.float32
bf16 = jnp.bfloat16
TAIL = 16


def dot(a, b, dim_a=1, dim_b=0):
    return lax.dot_general(a, b, (((dim_a,), (dim_b,)), ((), ())), preferred_element_type=f32)


def kernel(fn, name, outs, ins, flops=0, scalars=0):
    count = len(ins)
    pairs = [i if isinstance(i, tuple) else (i, None) for i in ins]

    def run(*refs):
        views = [r if at is None else r.at[at] for r, (_, at) in zip(refs[:count], pairs)]
        fn(views, refs[count:])

    whole = pl.BlockSpec(memory_space=pltpu.VMEM)
    return pl.pallas_call(
        run,
        out_shape=tuple(jax.ShapeDtypeStruct(s, t) for s, t in outs),
        in_specs=[pl.BlockSpec(memory_space=pltpu.SMEM)] * scalars + [whole] * (count - scalars),
        out_specs=tuple(whole for _ in outs),
        compiler_params=pltpu.CompilerParams(vmem_limit_bytes=24 << 20),
        cost_estimate=pl.CostEstimate(flops=flops, transcendentals=0, bytes_accessed=0),
        name=name,
    )(*[a for a, _ in pairs])


def spans(width, step=256):
    return [(i, min(step, width - i)) for i in range(0, width, step)]


def square_rows(x):
    wide = x.astype(f32)
    ones = jnp.ones((8, x.shape[1]), bf16)
    return two_parts(dot(ones, (wide * wide).astype(bf16), 1, 1))


def two_parts(row):
    high = row.astype(bf16).astype(f32)
    return jnp.concatenate([high, row - high], axis=0).astype(bf16)


def joined(tail):
    wide = tail.astype(f32)
    return wide[:8] + wide[8:]


def as_column(row):
    size = row.shape[1]
    spread = jnp.broadcast_to(row[0:1], (size, size))
    at = lax.broadcasted_iota(jnp.int32, (size, size), 0)
    across = lax.broadcasted_iota(jnp.int32, (size, size), 1)
    return jnp.sum(jnp.where(at == across, spread, 0.0), axis=1, keepdims=True)


def sigmoid(v):
    return 1.0 / (1.0 + jnp.exp(-v))


def slope(pre):
    sig = sigmoid(pre)
    return sig * (1.0 + pre * (1.0 - sig))


def added(own, other, rows):
    return own[0:rows, :].astype(f32) + other[0:rows, :].astype(f32)


def middle(owns, others, tails):
    def fn(ins, outs):
        half = len(outs)
        for own, other, out, tail in zip(ins[:half], ins[half:], outs, tails):
            rows = own.shape[0] - (TAIL if tail else 0)
            out[0:rows, :] = added(own, other, rows).astype(bf16)
            if tail:
                out[rows:, :] = two_parts(joined(own[rows:, :]) + joined(other[rows:, :]))

    return kernel(fn, "middle", [(p.shape, bf16) for p in owns], list(owns) + list(others))


def pair_sums(parts, axis, tails):
    size = lax.axis_size(axis)
    if size & (size - 1) or size == 1:
        return [(lax.psum(p.astype(f32), axis).astype(bf16), jnp.zeros_like(p)) for p in parts]
    stride = 1
    while True:
        pairs = [(i, i ^ stride) for i in range(size)]
        others = [lax.ppermute(p, axis, pairs) for p in parts]
        stride *= 2
        if stride == size:
            return list(zip(parts, others))
        parts = middle(parts, others, tails)


def ring_order(size):
    return list(range(0, size, 2)) + list(range(size - 1 - size % 2, 0, -2))


def shard_of(a, k, size):
    rows = a.shape[0] // size
    return lax.dynamic_slice_in_dim(a, (k % size) * rows, rows, 0)


def ring_average(arrays, outs, axis):
    size = lax.axis_size(axis)
    if size > LONG_RING or any(a.shape[0] % (size * 16) for a in arrays):
        results = []
        for a, o in zip(arrays, outs):
            total = lax.psum_scatter(a.astype(f32).reshape(-1), axis, scatter_dimension=0, tiled=True)
            mean = (total / size).astype(bf16)
            whole = lax.all_gather(mean, axis, axis=0, tiled=True)
            results.append(whole.reshape(a.shape).astype(o))
        return results
    order = ring_order(size)
    place = [0] * size
    for k, d in enumerate(order):
        place[d] = k
    me = jnp.asarray(place, jnp.int32)[lax.axis_index(axis)]
    ahead = [(order[k], order[(k + 1) % size]) for k in range(size)]
    back = [(b, a) for a, b in ahead]
    ways = [(ahead, 1) if j % 2 == 0 else (back, -1) for j in range(len(arrays))]

    held = [shard_of(a, me - sign, size) for a, (_, sign) in zip(arrays, ways)]
    for hop in range(1, size):
        moved = [lax.ppermute(h, axis, way) for h, (way, _) in zip(held, ways)]
        held = []
        for m, a, (_, sign) in zip(moved, arrays, ways):
            total = m.astype(f32) + shard_of(a, me - sign * (hop + 1), size).astype(f32)
            if hop == size - 1:
                total = total / size
            held.append(total.astype(bf16))
    pieces = [[h] for h in held]
    for hop in range(1, size):
        held = [lax.ppermute(h, axis, way) for h, (way, _) in zip(held, ways)]
        for row, h in zip(pieces, held):
            row.append(h)

    def fn(ins, results):
        at = ins[0][0]
        for j, (out, (_, sign)) in enumerate(zip(results, ways)):
            rows = out.shape[0] // size
            for hop in range(size):
                start = pl.multiple_of(((at + size - sign * hop) % size) * rows, 16)
                out[pl.ds(start, rows), :] = ins[1 + j * size + hop][...].astype(out.dtype)

    return kernel(
        fn,
        "gathered",
        [(a.shape, o) for a, o in zip(arrays, outs)],
        [me.reshape(1)] + [p for row in pieces for p in row],
        scalars=1,
    )


def body(hidden, target, w_down, w_up, m_down, m_up):
    tokens, local = hidden.shape[1:]
    rank = w_down.shape[3]
    width = local * lax.axis_size("ta")
    cd, cu = width**-0.5, rank**-0.5
    chunks = spans(local)
    sq = (tokens, rank)
    thin = (tokens, 128)
    x0, goal = (hidden, 0), (target, 0)
    wd0, wd1 = [(w_down, (0, k)) for k in range(2)]
    wu0, wu1 = [(w_up, (0, k)) for k in range(2)]
    md0, md1 = [(m_down, (0, k)) for k in range(2)]
    mu0, mu1 = [(m_up, (0, k)) for k in range(2)]
    unit = 2 * tokens * rank * local

    def rms_of(row):
        return jnp.sqrt(as_column(row) / width + norm_eps)

    def activation(pre):
        return (pre * sigmoid(pre)).astype(bf16)

    def lift(out, base, act, weights):
        for i, n in chunks:
            up = dot(act, weights[:, i : i + n]) * cu
            out[:, i : i + n] = (base[:, i : i + n].astype(f32) + up).astype(bf16)

    def into_layer1(pay, x1, wd1):
        pay[0:tokens, :] = dot(x1[...], wd1[...]).astype(bf16)
        pay[tokens:, :] = square_rows(x1[...])

    def step_up(m, w, new_m, new_w, act, grad):
        for i, n in chunks:
            moment = moment_decay * m[:, i : i + n] + dot(act, grad(i, n), 0, 0) * cu
            new_m[:, i : i + n] = moment.astype(new_m.dtype)
            new_w[:, i : i + n] = (w[:, i : i + n].astype(f32) - learn_rate * moment).astype(bf16)

    def step_down(m, w, new_m, new_w, x, g_proj):
        for i, n in chunks:
            moment = moment_decay * m[i : i + n, :] + dot(x[:, i : i + n], g_proj, 0, 0) * cd
            new_m[i : i + n, :] = moment.astype(new_m.dtype)
            new_w[i : i + n, :] = (w[i : i + n, :].astype(f32) - learn_rate * moment).astype(bf16)

    def last_grad(x2, goal, i, n):
        return x2[:, i : i + n].astype(f32) - goal[:, i : i + n].astype(f32)

    def layer1_back(a1, b1, pre1, rms1):
        g_act = added(a1, b1, tokens) * cu
        pre, rms = pre1[...], rms1[:, 0:1]
        g_pre = g_act * slope(pre)
        row_dot = jnp.sum(g_pre * pre, axis=1, keepdims=True)
        return (g_pre / rms).astype(bf16), row_dot / (width * rms * rms)

    def mid_grad(g_proj, pull, x1, x2, goal, wd1, i, n):
        through = dot(g_proj, wd1[i : i + n, :], 1, 1) * cd
        return last_grad(x2, goal, i, n) + through - pull * x1[:, i : i + n].astype(f32)

    def layer0_back(a0, b0, gh, hg, g_proj1, pull, proj0, rms0):
        cross = (gh[0:tokens, :].astype(f32) + hg[0:tokens, :].astype(f32)).astype(bf16)
        low = gh[tokens:, :].astype(f32) + hg[tokens:, :].astype(f32)
        g_act = (added(a0, b0, tokens) + dot(g_proj1, cross, 1, 1) * cd - pull * low) * cu
        rms = rms0[:, 0:1]
        return (g_act * slope(proj0[...] * (cd / rms)) / rms).astype(bf16)

    def fn_init(ins, outs):
        x0, wd0, md0 = ins
        pay = outs[0]
        x = x0[...]
        pay[0:tokens, :] = dot(x, wd0[...]).astype(bf16)
        pay[tokens : 2 * tokens, :] = dot(x, md0[...].astype(bf16)).astype(bf16)
        pay[2 * tokens : 3 * tokens, :] = dot(x, x, 1, 1).astype(bf16)
        pay[3 * tokens :, :] = square_rows(x)

    (pay,) = kernel(
        fn_init,
        "init",
        [((3 * tokens + TAIL, rank), bf16)],
        [x0, wd0, md0],
        3 * unit,
    )
    ((own, other),) = pair_sums([pay], "ta", [True])

    def fn_enter(ins, outs):
        own, other, x0, wu0, wd1 = ins
        proj0, drift0, gram0, rms0, act0, x1, pay = outs
        total = added(own, other, 3 * tokens)
        proj = total[0:tokens]
        proj0[...] = proj
        drift0[...] = total[tokens : 2 * tokens]
        gram0[...] = total[2 * tokens :].astype(bf16)
        rms = rms_of(joined(own[3 * tokens :, :]) + joined(other[3 * tokens :, :]))
        rms0[...] = jnp.broadcast_to(rms, thin)
        act = activation(proj * (cd / rms))
        act0[...] = act
        lift(x1, x0, act, wu0)
        into_layer1(pay, x1, wd1)

    proj0, drift0, gram0, rms0, act0, x1, pay = kernel(
        fn_enter,
        "enter",
        [
            (sq, f32),
            (sq, f32),
            (sq, bf16),
            (thin, f32),
            (sq, bf16),
            ((tokens, local), bf16),
            ((tokens + TAIL, rank), bf16),
        ],
        [own, other, x0, wu0, wd1],
        2 * unit,
    )

    def crosses(pay, x1, wu0, wd1):
        pay[0:rank, :] = dot(wu0[...], wd1[...]).astype(bf16)
        pay[rank:, :] = dot(x1[...], wu0[...], 1, 1).astype(bf16)

    def fn_cross(ins, outs):
        crosses(outs[0], *ins)

    pay_c = kernel(
        fn_cross,
        "cross",
        [((rank + tokens, rank), bf16)],
        [x1, wu0, wd1],
        2 * unit,
    )[0]

    down = ((local, rank), bf16)
    up = ((rank, local), bf16)
    down_m = ((local, rank), f32)
    up_m = ((rank, local), f32)

    def fn_second(ins, outs):
        own, other, x1, wu1, wu0, goal = ins
        pre1, rms1, act1, x2, a1, a0 = outs
        rms = rms_of(joined(own[tokens:, :]) + joined(other[tokens:, :]))
        pre = added(own, other, tokens) * (cd / rms)
        pre1[...] = pre
        rms1[...] = jnp.broadcast_to(rms, thin)
        act = activation(pre)
        act1[...] = act
        lift(x2, x1, act, wu1)
        gb = (x2[...].astype(f32) - goal[...].astype(f32)).astype(bf16)
        a1[...] = dot(gb, wu1[...], 1, 1).astype(bf16)
        a0[...] = dot(gb, wu0[...], 1, 1).astype(bf16)

    def fn_back1(ins, outs):
        a1, b1, pre1, rms1, act0, x1, x2, goal, wd1, wu0, md1, mu0 = ins
        g_proj1, pull1, new_md1, new_wd1, new_mu0, new_wu0 = outs
        g_proj, pull = layer1_back(a1, b1, pre1, rms1)
        g_proj1[...] = g_proj
        pull1[...] = jnp.broadcast_to(pull, thin)
        step_up(
            mu0, wu0, new_mu0, new_wu0, act0[...],
            lambda i, n: mid_grad(g_proj, pull, x1, x2, goal, wd1, i, n).astype(bf16),
        )
        step_down(md1, wd1, new_md1, new_wd1, x1, g_proj)

    def fn_back0(ins, outs):
        a0, b0, gh, hg, g_proj1, pull1, proj0, rms0, drift0, gram0, x0, wu0, wd1 = ins
        g_proj0, new_proj0, new_drift0, act0, x1, pay = outs
        g_proj = layer0_back(a0, b0, gh, hg, g_proj1[...], pull1[:, 0:1], proj0, rms0)
        g_proj0[...] = g_proj
        drift = moment_decay * drift0[...] + dot(gram0[...], g_proj) * cd
        proj = proj0[...] - learn_rate * drift
        new_drift0[...] = drift
        new_proj0[...] = proj
        act = activation(proj * (cd / rms0[:, 0:1]))
        act0[...] = act
        lift(x1, x0, act, wu0)
        into_layer1(pay, x1, wd1)

    def fn_rest(ins, outs):
        x1, wu0, wd1, act1, x2, goal, mu1, wu1, x0, g_proj0, md0, wd0 = ins
        pay, new_mu1, new_wu1, new_md0, new_wd0 = outs
        crosses(pay, x1, wu0, wd1)
        step_up(
            mu1, wu1, new_mu1, new_wu1, act1[...],
            lambda i, n: last_grad(x2, goal, i, n).astype(bf16),
        )
        step_down(md0, wd0, new_md0, new_wd0, x0, g_proj0[...])

    def fn_last(ins, outs):
        (a1, b1, a0, b0, gh, hg, pre1, rms1, proj0, rms0, act0, act1, x0, x1, x2, goal) = ins[:16]
        wd0, wd1, wu0, wu1, md0, md1, mu0, mu1 = ins[16:]
        wd, wu, md, mu = outs
        g_proj1, pull = layer1_back(a1, b1, pre1, rms1)
        g_proj0 = layer0_back(a0, b0, gh, hg, g_proj1, pull, proj0, rms0)

        def half(ref, k):
            rows = ref.shape[0] // 2
            return ref.at[k * rows : (k + 1) * rows, :]

        step_up(
            mu0, wu0, half(mu, 0), half(wu, 0), act0[...],
            lambda i, n: mid_grad(g_proj1, pull, x1, x2, goal, wd1, i, n).astype(bf16),
        )
        step_up(
            mu1, wu1, half(mu, 1), half(wu, 1), act1[...],
            lambda i, n: last_grad(x2, goal, i, n).astype(bf16),
        )
        step_down(md0, wd0, half(md, 0), half(wd, 0), x0, g_proj0)
        step_down(md1, wd1, half(md, 1), half(wd, 1), x1, g_proj1)

    for step in range(STEPS):
        ((own, other),) = pair_sums([pay], "ta", [True])
        ((gh, hg),) = pair_sums([pay_c], "ta", [False])
        pre1, rms1, act1, x2, a1, a0 = kernel(
            fn_second,
            "second",
            [(sq, f32), (thin, f32), (sq, bf16), ((tokens, local), bf16), (sq, bf16), (sq, bf16)],
            [own, other, x1, wu1, wu0, goal],
            3 * unit,
        )
        (a1, b1), (a0, b0) = pair_sums([a1, a0], "ta", [False, False])
        if step == STEPS - 1:
            break
        g_proj1, pull1, md1, wd1, mu0, wu0 = kernel(
            fn_back1,
            "back1",
            [(sq, bf16), (thin, f32), down_m, down, up_m, up],
            [a1, b1, pre1, rms1, act0, x1, x2, goal, wd1, wu0, md1, mu0],
            3 * unit,
        )
        g_proj0, proj0, drift0, act0, x1, pay = kernel(
            fn_back0,
            "back0",
            [
                (sq, bf16), (sq, f32), (sq, f32), (sq, bf16), ((tokens, local), bf16),
                ((tokens + TAIL, rank), bf16),
            ],
            [a0, b0, gh, hg, g_proj1, pull1, proj0, rms0, drift0, gram0, x0, wu0, wd1],
            2 * unit,
        )
        pay_c, mu1, wu1, md0, wd0 = kernel(
            fn_rest,
            "rest",
            [((rank + tokens, rank), bf16), up_m, up, down_m, down],
            [x1, wu0, wd1, act1, x2, goal, mu1, wu1, x0, g_proj0, md0, wd0],
            4 * unit,
        )

    ends = [((2 * local, rank), bf16), ((2 * rank, local), bf16)]
    wd, wu, md, mu = kernel(
        fn_last,
        "last",
        ends + ends,
        [a1, b1, a0, b0, gh, hg, pre1, rms1, proj0, rms0, act0, act1, x0, x1, x2, goal]
        + [wd0, wd1, wu0, wu1, md0, md1, mu0, mu1],
        5 * unit,
    )
    wd, wu, md, mu = ring_average([wd, wu, md, mu], [bf16, bf16, f32, f32], "row")
    down, up = w_down.shape[1:], w_up.shape[1:]
    return (wd.reshape(down), wu.reshape(up), md.reshape(down), mu.reshape(up))


def solution(mesh):
    placed = (
        P("row", None, "ta"),
        P("row", None, "ta"),
        P("row", None, "ta", None),
        P("row", None, None, "ta"),
        P("row", None, "ta", None),
        P("row", None, None, "ta"),
    )
    return jax.shard_map(
        body,
        mesh=mesh,
        in_specs=placed,
        out_specs=(
            P(None, "ta", None),
            P(None, None, "ta"),
            P(None, "ta", None),
            P(None, None, "ta"),
        ),
        check_vma=False,
    )
```
